32 devices in a mesh: grp: 2 (over y), kv: 8 (over z, core), hd: 2 (over x), sub: 1.
Axes of the slice: x: 2, y: 2, z: 4, core: 2. Of those that a mesh axis runs over, the one named last changes fastest.
Arguments:
- queries: bfloat16 [256, 8192], P(('grp', 'kv'), 'hd'), parts along dimension 0, may hold values from -12 to 12
- prompt_of: int32 [256, 1], P('grp'), parts along dimension 0, may hold values from 0 to 1; in each aligned block of 16 rows (0 to 15, 16 to 31, ...) at most 8 rows name the same one
- prompt_len: int32 [4], P('grp'), parts along dimension 0, may hold values from 3072 to 4096
- suffix_len: int32 [256], P(('grp', 'kv')), parts along dimension 0, may hold values from 0 to 512
- page_table: int32 [256, 8], P(('grp', 'kv'), 'sub'), parts along dimension 0, may hold values from 0 to 127, as said below
- prompt_keys: bfloat16 [16384, 1024], P(('grp', 'kv', 'sub'), 'hd'), parts along dimension 0, may hold values from -14 to 14
- shared_prompt_values: bfloat16 [16384, 1024], P(('grp', 'kv', 'sub'), 'hd'), parts along dimension 0, may hold values from -6 to 6
- suffix_pool_keys: bfloat16 [2048, 64, 1024], P(('grp', 'kv', 'sub'), None, 'hd'), parts along dimension 0, may hold values from -14 to 14
- suffix_pool_values: bfloat16 [2048, 64, 1024], P(('grp', 'kv', 'sub'), None, 'hd'), parts along dimension 0, may hold values from -6 to 6
Outputs:
- attended: float32 [256, 8192], P(('grp', 'kv'), 'hd'), parts along dimension 0
The draws below stay inside these ranges and needn't reach their ends.
There are 2 independent parts, one for each index of `grp`. The reference program is written for one: setup_inputs(seed, part) draws one part's arguments, and reference() takes and returns one part's arrays. A program takes and returns all parts, laid end to end along the dimension named above; each array names one. Nothing has to cross between parts.
Inputs may be any that keep to these rules, and one draw needn't show every extreme that they name: `prompt_of`: in each aligned block of 16 rows (the sequences of one index of kv), every prompt is named by exactly 8 rows. `page_table`: for each index k of kv and s of sub, the entries in rows k * 16 to (k + 1) * 16 - 1 and columns s * 8 to (s + 1) * 8 - 1 are a permutation of 0 to 127.
All inputs are finite; a program needn't handle non-finite values.
Results may differ from the reference program's by a relative error of at most 0.0011.
Values may be sent and summed in bfloat16 or wider, within the bound.
No kernel may reach another device: no remote copies, remote signals or barrier semaphores. Data moves between devices by JAX's collectives and lax.ppermute only.
A program may use at most 128 MiB of HBM per device.

```python
import math
import jax
import jax.numpy as jnp
import numpy as np
from jax import lax

QUERY_HEADS = 64
KEY_VALUE_HEADS = 8
HEAD_SIZE = 128
SEQ_DEV = 16
CACHE_PER_DEVICE = 1024
SUF_MAX = 512
PAGE_POSITIONS = 64
SEQS = 128
REACH = 1024
PROMPT_TOKENS = 8192
PROMPTS = 2
MOST = 8
PAGES_SEQ = 8
HALF_PAGE_SLOTS = 8
POOL_DEV = 128
POOL_PAGES = 1024
N_KV = 8
N_SUB = 1


def offset_key_rows(key, salt, array_shape):
    sampled_array = 2.5 * jax.random.truncated_normal(jax.random.fold_in(key, salt), -4.8, 4.8, array_shape, jnp.float32)
    return sampled_array


def draw_prompt_keys(key, part):
    return offset_key_rows(key, 17, (PROMPT_TOKENS, KEY_VALUE_HEADS * HEAD_SIZE)).astype(jnp.bfloat16)


def draw_suffix_pool_keys(key, part):
    return offset_key_rows(key, 19, (POOL_PAGES, PAGE_POSITIONS, KEY_VALUE_HEADS * HEAD_SIZE)).astype(jnp.bfloat16)


def draw_queries(key, part):
    sampled_array = jax.random.truncated_normal(jax.random.fold_in(key, 29), -6.0, 6.0, (SEQS, QUERY_HEADS * HEAD_SIZE), jnp.float32)
    return sampled_array.astype(jnp.bfloat16)


def local_order(block_key):
    return jax.random.permutation(block_key, POOL_DEV)


def draw_page_table(key, part):
    block_keys = jax.random.split(jax.random.fold_in(key, 41), N_KV * N_SUB)
    orders = jax.vmap(local_order)(block_keys).astype(jnp.int32)
    orders = orders.reshape(N_KV, N_SUB, SEQ_DEV, HALF_PAGE_SLOTS).transpose(0, 2, 1, 3)
    return orders.reshape(SEQS, PAGES_SEQ).astype(jnp.int32)


def set_ends(entries, stream_key, low, high):
    longest = entries.shape.index(max(entries.shape))
    spots = []
    for shift in (0, 1):
        where = [jax.random.randint(jax.random.fold_in(stream_key, axis), (), 0, length) for axis, length in enumerate(entries.shape)]
        where[longest] = (where[longest] + shift) % entries.shape[longest]
        spots.append(tuple(where))
    return entries.at[spots[0]].set(low).at[spots[1]].set(high)


def level_of(own_key, dims, cuts, low, high):
    def one(dim, shards_of):
        heights = jax.random.uniform(jax.random.fold_in(jax.random.fold_in(own_key, 6), dim), (shards_of,), jnp.float32, low / len(cuts), high / len(cuts))
        return jnp.repeat(jnp.exp(heights), dims[dim] // shards_of).reshape((-1,) + (1,) * (len(dims) - dim - 1))

    loudness = one(*cuts[0])
    for cut in cuts[1:]:
        loudness = loudness * one(*cut)
    return loudness


def deal_out(stream_key, own, number, rows, count, top, limit, slope):
    order = jax.random.permutation(stream_key, count)
    heavy_load, common = portions_of(count, rows * top, limit, slope, True), portions_of(count, rows * top, limit, slope, False)
    places = jnp.arange(count)

    def named(sizes, turn):
        used = int((sizes > 0).sum())
        fixed = max(1, used // 4)
        shifted = fixed + (places - fixed + turn * (used - fixed)) % max(1, count - fixed)
        return jnp.zeros((count,), jnp.int32).at[order[jnp.where(places < fixed, places, shifted)]].set(jnp.asarray(sizes, jnp.int32))

    sizes = jnp.where(number % 4 == 0, named(heavy_load, number // 4), named(common, number - number // 4 - 1))
    mixed = jax.random.permutation(jax.random.fold_in(own, 3), count)
    source_of, taker = mixed[0:count // 2 * 2:2], mixed[1:count // 2 * 2:2]
    room = jnp.minimum(sizes[source_of] - 1, limit - sizes[taker]) // 2
    room = jnp.where((source_of == order[0]) | (taker == order[0]) | (sizes[taker] == 0), 0, jnp.maximum(room, 0))
    shifted = jax.random.randint(jax.random.fold_in(own, 4), (count // 2,), 0, 1 << 20) % (room + 1)
    sizes = sizes.at[source_of].add(-shifted).at[taker].add(shifted)
    items = jnp.searchsorted(jnp.cumsum(sizes), jnp.arange(rows * top), side="right").astype(jnp.int32)
    table = items.reshape(top, rows).T
    table = table[jax.random.permutation(jax.random.fold_in(own, 1), rows)]
    turn = jax.random.randint(jax.random.fold_in(own, 2), (rows, 1), 0, top)
    return jnp.take_along_axis(table, (jnp.arange(top)[None, :] + turn) % top, axis=1)


def portions_of(count, total, most, skew, full):
    loads = [(1 << 20) // math.isqrt(rank ** skew) + 1 for rank in range(1, count + 1)]
    largest = most if full else min(most, max(-(-total // count), total * loads[0] // sum(loads)))
    least = 1 if total - largest >= count - 1 else 0
    given, rest = [largest] + [least] * (count - 1), total - largest - least * (count - 1)
    while rest > 0:
        candidates = [i for i in range(1, count) if given[i] < largest] or [i for i in range(1, count) if given[i] < most]
        mass, left = sum([loads[i] for i in candidates]), rest
        for i in candidates:
            extra = min(most - given[i], max(1, left * loads[i] // mass), rest)
            given[i] = given[i] + extra
            rest = rest - extra
    return np.array(given)


def scatter_about(rng, extent, scale, limit, pieces=(), held_as=jnp.bfloat16):
    array = jax.random.normal(rng, extent, jnp.float32) * scale
    if len(pieces) > 0:
        array = level_of(rng, extent, pieces, -0.22, 0.18) * array
    return jnp.clip(array, min=-limit, max=limit).astype(held_as)


def setup_inputs(seed: int = 0, part: int = 0) -> dict:
    arg_keys = jax.random.split(jax.random.key(seed), 10)
    part_splits = jax.random.split(jax.random.fold_in(arg_keys[9], part), 10)
    queries = draw_queries(jax.random.fold_in(jax.random.fold_in(arg_keys[9], part), 71), part)
    prompt_of_keys = jax.random.split(jax.random.fold_in(part_splits[1], 1), SEQS // SEQ_DEV)
    prompt_of_turns = jax.random.permutation(jax.random.fold_in(part_splits[1], 3), SEQS // SEQ_DEV)
    prompt_of = jax.vmap(lambda own, number: deal_out(jax.random.fold_in(part_splits[1], 2), own, number, SEQ_DEV, PROMPTS, 1, MOST, 2))(prompt_of_keys, prompt_of_turns).reshape((SEQS, 1))
    prompt_len = jax.random.randint(part_splits[2], (PROMPTS,), 3 * REACH, 4 * REACH + 1).astype(jnp.int32)
    suffix_len = set_ends(jax.random.randint(part_splits[3], (SEQS,), 0, SUF_MAX + 1), jax.random.fold_in(part_splits[3], 1), 0, SUF_MAX).astype(jnp.int32)
    page_table = draw_page_table(jax.random.fold_in(jax.random.fold_in(arg_keys[9], part), 71), part)
    prompt_keys = draw_prompt_keys(jax.random.fold_in(jax.random.fold_in(arg_keys[9], part), 71), part)
    shared_prompt_values = scatter_about(part_splits[6], (PROMPT_TOKENS, KEY_VALUE_HEADS * HEAD_SIZE), 1.0, 6.0, ((0, 8), (1, 2)))
    suffix_pool_keys = draw_suffix_pool_keys(jax.random.fold_in(jax.random.fold_in(arg_keys[9], part), 71), part)
    suffix_pool_values = scatter_about(part_splits[8], (POOL_PAGES, PAGE_POSITIONS, KEY_VALUE_HEADS * HEAD_SIZE), 1.0, 6.0, ((0, 8), (2, 2)))
    return {"queries": queries, "prompt_of": prompt_of, "prompt_len": prompt_len, "suffix_len": suffix_len, "page_table": page_table, "prompt_keys": prompt_keys, "shared_prompt_values": shared_prompt_values, "suffix_pool_keys": suffix_pool_keys, "suffix_pool_values": suffix_pool_values}


NEGATIVE = -1e+30

def partial_blocks(query_head_rows, key_blocks, value_blocks, key_mask):
    scores = jnp.einsum('kgd,bckd->bkgc', query_head_rows, key_blocks, precision=lax.Precision.HIGHEST)
    scores = scores * (1.0 / math.sqrt(HEAD_SIZE))
    keeper = key_mask[:, None, None, :]
    scores = jnp.where(keeper, scores, NEGATIVE)
    row_max = lax.optimization_barrier(jnp.max(scores, axis=3, keepdims=True))
    weights = jnp.where(keeper, jnp.exp(scores - row_max), 0.0)
    totals = jnp.maximum(lax.optimization_barrier(jnp.sum(weights, axis=3)), 1.0)
    rounded = lax.optimization_barrier(weights.astype(jnp.bfloat16)).astype(jnp.float32)
    blended = jnp.einsum('bkgc,bckd->bkgd', rounded, value_blocks, precision=lax.Precision.HIGHEST)
    return (blended / totals[..., None], row_max[..., 0] + jnp.log(totals))

def reference(queries, prompt_of, prompt_len, suffix_len, page_table, prompt_keys, shared_prompt_values, suffix_pool_keys, suffix_pool_values):
    query_group_size = QUERY_HEADS // KEY_VALUE_HEADS
    block_count = N_KV * N_SUB
    slice_window = min(4 * N_SUB + 1, block_count)
    starts = (jnp.cumsum(prompt_len) - prompt_len).astype(jnp.int32)

    def one_sequence(page_index_value):
        prompt = prompt_of[page_index_value, 0]
        begin = starts[prompt]
        finish = begin + prompt_len[prompt]
        first_block = jnp.minimum(begin // CACHE_PER_DEVICE, block_count - slice_window).astype(jnp.int32)
        offset = (first_block * CACHE_PER_DEVICE).astype(jnp.int32)
        key_slice_window = lax.dynamic_slice_in_dim(prompt_keys, offset, slice_window * CACHE_PER_DEVICE, 0)
        value_slice_window = lax.dynamic_slice_in_dim(shared_prompt_values, offset, slice_window * CACHE_PER_DEVICE, 0)
        key_slice_window = key_slice_window.astype(jnp.float32).reshape(slice_window, CACHE_PER_DEVICE, KEY_VALUE_HEADS, HEAD_SIZE)
        value_slice_window = value_slice_window.astype(jnp.float32).reshape(slice_window, CACHE_PER_DEVICE, KEY_VALUE_HEADS, HEAD_SIZE)
        position = offset + jnp.arange(slice_window * CACHE_PER_DEVICE, dtype=jnp.int32).reshape(slice_window, CACHE_PER_DEVICE)
        prompt_mask = (position >= begin) & (position < finish)
        query_head_rows = queries[page_index_value].astype(jnp.float32).reshape(KEY_VALUE_HEADS, query_group_size, HEAD_SIZE)
        prompt_out, prompt_lse = partial_blocks(query_head_rows, key_slice_window, value_slice_window, prompt_mask)
        owner = (page_index_value // SEQ_DEV).astype(jnp.int32)
        slot_half = (jnp.arange(PAGES_SEQ, dtype=jnp.int32) // HALF_PAGE_SLOTS).astype(jnp.int32)
        page_list = (owner * N_SUB + slot_half) * POOL_DEV + page_table[page_index_value]
        suffix_page_block = suffix_pool_keys[page_list].astype(jnp.float32).reshape(N_SUB, HALF_PAGE_SLOTS * PAGE_POSITIONS, KEY_VALUE_HEADS, HEAD_SIZE)
        suffix_value_rows = suffix_pool_values[page_list].astype(jnp.float32).reshape(N_SUB, HALF_PAGE_SLOTS * PAGE_POSITIONS, KEY_VALUE_HEADS, HEAD_SIZE)
        suffix_pos = jnp.arange(PAGES_SEQ * PAGE_POSITIONS, dtype=jnp.int32).reshape(N_SUB, HALF_PAGE_SLOTS * PAGE_POSITIONS)
        suffix_mask = suffix_pos < suffix_len[page_index_value]
        suffix_out, suffix_lse = partial_blocks(query_head_rows, suffix_page_block, suffix_value_rows, suffix_mask)
        every_lse = jnp.concatenate([prompt_lse, suffix_lse], axis=0)
        every_out = jnp.concatenate([prompt_out, suffix_out], axis=0)
        joint_max = lax.optimization_barrier(jnp.max(every_lse, axis=0))
        factors = jnp.exp(every_lse - joint_max)
        merged = lax.optimization_barrier(jnp.sum(factors[..., None] * every_out, axis=0)) / lax.optimization_barrier(jnp.sum(factors, axis=0))[..., None]
        return merged.reshape(QUERY_HEADS * HEAD_SIZE)
    result = lax.map(one_sequence, jnp.arange(SEQS, dtype=jnp.int32))
    return result.astype(jnp.float32)
```

```python
import functools
import math

import jax
import jax.numpy as jnp
from jax import lax
from jax.experimental import pallas as pl
from jax.experimental.pallas import tpu as pltpu
from jax.sharding import PartitionSpec as P

HEAD_SIZE = 128


NEGATIVE = -1e30


def joined(value, axis, combine):
    everything = jax.tree.map(lambda part: lax.all_gather(part, axis), value)
    leading = jax.tree.map(lambda part: part[0], everything)

    def hop(k, so_far):
        return combine(so_far, jax.tree.map(lambda part: part[k], everything))

    return lax.fori_loop(1, lax.axis_size(axis), hop, leading)


def attend_block(sent_rows, key_block, value_block, lower_bound, upper_bound, first_position):
    row_count = sent_rows.shape[0]
    key_count = key_block.shape[0]
    kv_local = key_block.shape[1] // HEAD_SIZE
    query_group_size = sent_rows.shape[1] // (HEAD_SIZE * kv_local)
    position = first_position + jnp.arange(key_count, dtype=jnp.int32)
    key_mask = (position[None, :] >= lower_bound[:, None]) & (
        position[None, :] < upper_bound[:, None]
    )
    key_mask = key_mask[:, None, :]
    score_scale = 1.0 / math.sqrt(HEAD_SIZE)
    blended_parts = []
    lse_parts = []
    for kv_head in range(kv_local):
        low_column = kv_head * query_group_size * HEAD_SIZE
        head_query = sent_rows[:, low_column : low_column + query_group_size * HEAD_SIZE].reshape(
            row_count * query_group_size, HEAD_SIZE
        )
        head_keys = key_block[:, kv_head * HEAD_SIZE : (kv_head + 1) * HEAD_SIZE]
        head_values = value_block[:, kv_head * HEAD_SIZE : (kv_head + 1) * HEAD_SIZE]
        scores = lax.dot_general(
            head_query, head_keys, (((1,), (1,)), ((), ())), preferred_element_type=jnp.float32
        )
        scores = (scores * score_scale).reshape(row_count, query_group_size, key_count)
        scores = jnp.where(key_mask, scores, NEGATIVE)
        row_max = jnp.max(scores, axis=2, keepdims=True)
        weights = jnp.where(key_mask, jnp.exp(scores - row_max), 0.0)
        totals = jnp.maximum(jnp.sum(weights, axis=2), 1.0)
        weighted = jnp.dot(
            weights.astype(jnp.bfloat16).reshape(row_count * query_group_size, key_count),
            head_values,
            preferred_element_type=jnp.float32,
        )
        weighted = weighted.reshape(row_count, query_group_size, HEAD_SIZE) / totals[:, :, None]
        blended_parts.append(weighted.reshape(row_count, query_group_size * HEAD_SIZE))
        lse_parts.append(row_max[:, :, 0] + jnp.log(totals))
    return (jnp.concatenate(blended_parts, axis=1), jnp.concatenate(lse_parts, axis=1))


def combine_halves(earlier, later):
    joint_max = jnp.maximum(earlier[0], later[0])
    left_factor = jnp.exp(earlier[0] - joint_max)
    right_factor = jnp.exp(later[0] - joint_max)
    totals = earlier[1] * left_factor + later[1] * right_factor
    blended = earlier[2] * left_factor[:, :, None] + later[2] * right_factor[:, :, None]
    return (joint_max, totals, blended)


def shards(
    queries,
    prompt_of,
    prompt_len,
    suffix_len,
    page_table,
    prompt_keys,
    shared_prompt_values,
    suffix_pool_keys,
    suffix_pool_values,
):
    kv_count = lax.axis_size("kv")
    sub_count = lax.axis_size("sub")
    kv_index = lax.axis_index("kv")
    sub_index = lax.axis_index("sub")
    seq_local = queries.shape[0]
    row_width = queries.shape[1]
    heads_local = row_width // HEAD_SIZE
    cache_local = prompt_keys.shape[0]
    kv_reach = sub_count * cache_local
    prompt_count = prompt_len.shape[0]
    prompt_starts = jnp.cumsum(prompt_len) - prompt_len
    prompt_ends = prompt_starts + prompt_len
    prompt_labels = jnp.arange(prompt_count, dtype=jnp.int32)
    range_low = jnp.arange(kv_count, dtype=jnp.int32) * kv_reach
    intersections = (prompt_starts[None, :] < range_low[:, None] + kv_reach) & (
        prompt_ends[None, :] > range_low[:, None]
    )
    later_slot = prompt_starts[None, :] > range_low[:, None]
    first_position = (kv_index * sub_count + sub_index) * cache_local
    most_rows = seq_local // prompt_count
    owned_prompt = lax.dynamic_slice_in_dim(prompt_of[:, 0], kv_index * seq_local, seq_local)
    prompt_hits = owned_prompt[:, None] == prompt_labels[None, :]
    hit_counts = prompt_hits.astype(jnp.int32)
    ranks = jnp.sum((jnp.cumsum(hit_counts, axis=0) - hit_counts) * hit_counts, axis=1)
    seq_intersection = jnp.any(intersections[:, None, :] & prompt_hits[None, :, :], axis=2)
    seq_later = jnp.any(later_slot[:, None, :] & prompt_hits[None, :, :], axis=2).astype(jnp.int32)
    slot_labels = jnp.arange(2, dtype=jnp.int32)
    rank_labels = jnp.arange(most_rows, dtype=jnp.int32)
    selector = seq_intersection[:, None, None, :] & (
        seq_later[:, None, None, :] == slot_labels[None, :, None, None]
    )
    selector = selector & (ranks[None, None, None, :] == rank_labels[None, None, :, None])
    selector = selector.reshape(kv_count * 2 * most_rows, seq_local)
    outgoing = jnp.dot(
        selector.astype(jnp.bfloat16), queries, preferred_element_type=jnp.float32
    ).astype(jnp.bfloat16)
    incoming = lax.all_to_all(
        outgoing.reshape(kv_count, 2 * most_rows, row_width),
        "kv",
        split_axis=0,
        concat_axis=0,
        tiled=True,
    )
    mine_intersection = lax.dynamic_index_in_dim(intersections, kv_index, 0, keepdims=False)
    mine_later = lax.dynamic_index_in_dim(later_slot, kv_index, 0, keepdims=False).astype(jnp.int32)
    chosen = mine_intersection[None, :] & (mine_later[None, :] == slot_labels[:, None])
    slot_low = jnp.sum(jnp.where(chosen, prompt_starts[None, :], 0), axis=1)
    slot_high = jnp.sum(jnp.where(chosen, prompt_ends[None, :], 0), axis=1)
    lower_bound = jnp.broadcast_to(
        jnp.repeat(slot_low, most_rows)[None, :], (kv_count, 2 * most_rows)
    ).reshape(-1)
    upper_bound = jnp.broadcast_to(
        jnp.repeat(slot_high, most_rows)[None, :], (kv_count, 2 * most_rows)
    ).reshape(-1)
    sent_rows = incoming.reshape(kv_count * 2 * most_rows, row_width)
    back_rows = 2 * most_rows
    prompt_out, prompt_lse = attend_block(
        sent_rows, prompt_keys, shared_prompt_values, lower_bound, upper_bound, first_position
    )
    returned_out, returned_lse = (
        lax.all_to_all(
            prompt_out.reshape(kv_count, back_rows, row_width),
            "kv",
            split_axis=0,
            concat_axis=0,
            tiled=True,
        ),
        lax.all_to_all(
            prompt_lse.reshape(kv_count, back_rows, heads_local),
            "kv",
            split_axis=0,
            concat_axis=0,
            tiled=True,
        ),
    )
    page_slots = page_table.shape[1]
    page_length = suffix_pool_keys.shape[1]
    suffix_span = page_slots * page_length
    gathered_keys = suffix_pool_keys[page_table].reshape(seq_local, suffix_span, -1)
    gathered_values = suffix_pool_values[page_table].reshape(seq_local, suffix_span, -1)
    suffix_first = sub_index * suffix_span

    def one_sequence(query_line, seq_keys, seq_values, seq_length):
        return attend_block(
            query_line[None, :],
            seq_keys,
            seq_values,
            jnp.zeros((1,), jnp.int32),
            seq_length[None],
            suffix_first,
        )

    suffix_out, suffix_lse = jax.vmap(one_sequence)(
        queries, gathered_keys, gathered_values, suffix_len
    )
    suffix_out = suffix_out[:, 0].reshape(seq_local, heads_local, HEAD_SIZE)
    suffix_lse = suffix_lse[:, 0]
    flat_lse = returned_lse.reshape(-1, heads_local)
    flat_out = returned_out.reshape(-1, heads_local, HEAD_SIZE)
    masked_lse = jnp.where(selector[:, :, None], flat_lse[:, None, :], NEGATIVE)
    joint_max = jnp.maximum(jnp.max(masked_lse, axis=0), suffix_lse)
    factors = jnp.where(selector[:, :, None], jnp.exp(masked_lse - joint_max[None]), 0.0)
    own_factor = jnp.exp(suffix_lse - joint_max)
    totals = jnp.sum(factors, axis=0) + own_factor
    blended = jnp.einsum("rsh,rhd->shd", factors, flat_out, precision=lax.Precision.HIGHEST)
    blended = blended + own_factor[:, :, None] * suffix_out
    joint_max, totals, blended = joined((joint_max, totals, blended), "sub", combine_halves)
    return (blended / totals[:, :, None]).reshape(seq_local, row_width).astype(jnp.float32)


LANES = 128
WIRE = jnp.int16
WIRE_TOP = 32000.0
FRACTION_TOP = 32767.0
LOG2E = math.log2(math.e)


def dot_nt(a, b):
    return lax.dot_general(a, b, (((1,), (1,)), ((), ())), preferred_element_type=jnp.float32)


def packed_places(prompt_ref, seqs, group, visit):
    base = lax.axis_index("kv") * seqs
    half = seqs // 2
    front = jnp.int32(0)
    back = jnp.int32(half)
    for i in range(seqs):
        mine = prompt_ref[base + i] == group
        visit(i, jnp.where(mine, front, back))
        front = front + jnp.where(mine, 1, 0)
        back = back + jnp.where(mine, 0, 1)


def own_group():
    return lax.axis_index("kv") // (lax.axis_size("kv") // 2)


def pack_kernel(prompt_ref, q_ref, keep_ref, send_ref):
    seqs, width = q_ref.shape
    half = width // 2
    core = lax.axis_index("kv") % 2
    lane = lax.broadcasted_iota(jnp.int32, (seqs, LANES), 1)
    row = lax.broadcasted_iota(jnp.int32, (seqs, LANES), 0)
    place = jnp.full((seqs, LANES), -1, jnp.int32)
    dests = []
    packed_places(prompt_ref, seqs, own_group(), lambda i, d: dests.append(d))
    for i, d in enumerate(dests):
        place = jnp.where(lane == i, d, place)
    selector = jnp.where(place == row, 1.0, 0.0).astype(jnp.bfloat16)[:, :seqs]
    for ref, which in ((keep_ref, core), (send_ref, 1 - core)):
        block = q_ref[:, pl.ds(pl.multiple_of(which * half, LANES), half)]
        ref[...] = jnp.dot(selector, block, preferred_element_type=jnp.float32).astype(jnp.bfloat16)


def build_kernel(keep_ref, recv_ref, main_ref, cross_ref):
    rows = keep_ref.shape[0] // 2
    keep = keep_ref[...].astype(jnp.float32)
    recv = recv_ref[...].astype(jnp.float32)
    main_ref[...] = jnp.concatenate([keep[:rows], recv[:rows]], axis=0).astype(jnp.bfloat16)
    cross_ref[...] = jnp.concatenate([keep[rows:], recv[rows:]], axis=0).astype(jnp.bfloat16)


def suffix_kernel(
    first, prompt_ref, table_ref, length_ref, q_ref, k_hbm, v_hbm, o_ref, l_ref, order, kbuf, vbuf, ksem, vsem
):
    seqs, heads, head_size = q_ref.shape
    count, slots, page, width = kbuf.shape
    kv_heads = width // head_size
    group = heads // kv_heads
    span = slots * page

    def note(i, d):
        order[d] = jnp.int32(i)

    packed_places(prompt_ref, seqs, own_group(), note)
    for r in range(count):
        i = order[first + r]
        for j in range(slots):
            entry = table_ref[i, j]
            pltpu.make_async_copy(k_hbm.at[entry], kbuf.at[r, j], ksem.at[r]).start()
            pltpu.make_async_copy(v_hbm.at[entry], vbuf.at[r, j], vsem.at[r]).start()
    position = lax.broadcasted_iota(jnp.int32, (heads, span), 1)
    scale = 1.0 / math.sqrt(head_size)
    for r in range(count):
        i = order[first + r]
        pltpu.make_async_copy(kbuf.at[r], kbuf.at[r], ksem.at[r]).wait()
        pltpu.make_async_copy(vbuf.at[r], vbuf.at[r], vsem.at[r]).wait()
        q = q_ref[i]
        keys = kbuf[r].reshape(span, width)
        values = vbuf[r].reshape(span, width)
        scores = jnp.concatenate(
            [
                dot_nt(
                    q[h * group : (h + 1) * group], keys[:, h * head_size : (h + 1) * head_size]
                )
                for h in range(kv_heads)
            ],
            axis=0,
        )
        keep = position < length_ref[i]
        scores = jnp.where(keep, scores * scale, NEGATIVE)
        top = jnp.max(scores, axis=1, keepdims=True)
        weights = jnp.where(keep, jnp.exp(scores - top), 0.0)
        total = jnp.maximum(jnp.sum(weights, axis=1, keepdims=True), 1.0)
        rounded = weights.astype(jnp.bfloat16)
        out = jnp.concatenate(
            [
                jnp.dot(
                    rounded[h * group : (h + 1) * group],
                    values[:, h * head_size : (h + 1) * head_size],
                    preferred_element_type=jnp.float32,
                )
                for h in range(kv_heads)
            ],
            axis=0,
        )
        out = out / total
        lse = jnp.broadcast_to(top + jnp.log(total), (heads, head_size))
        for a in range(heads):
            columns = slice(a * head_size, (a + 1) * head_size)
            o_ref[r : r + 1, columns] = out[a : a + 1]
            l_ref[r : r + 1, columns] = lse[a : a + 1]


def prompt_kernel(
    core_ref, length_ref, *refs
):
    queries, extras = refs[0:4], refs[4:8]
    k_own, k_other, v_own, v_other = refs[8:12]
    own_out, outs, extra_outs = refs[12], refs[13:16], refs[16:20]
    kcat, vcat, qs, own_side, side, extra_side = refs[20:26]
    step = pl.program_id(0)
    rows, columns = queries[0].shape
    reach, head_size = k_own.shape
    group = columns // head_size
    heads = group * pl.num_programs(0)
    index = lax.axis_index("kv")
    core = index % 2
    chip = index // 2
    ours = own_group()
    first = chip * 2 * reach
    starts = (jnp.int32(0), length_ref[0])
    ends = (length_ref[0], length_ref[0] + length_ref[1])
    low = jnp.where(ours == 0, starts[0], starts[1])
    high = jnp.where(ours == 0, ends[0], ends[1])
    kcat[pl.ds(pl.multiple_of(core * reach, LANES), reach), :] = k_own[...]
    kcat[pl.ds(pl.multiple_of((1 - core) * reach, LANES), reach), :] = k_other[...]
    vcat[pl.ds(pl.multiple_of(core * reach, LANES), reach), :] = v_own[...]
    vcat[pl.ds(pl.multiple_of((1 - core) * reach, LANES), reach), :] = v_other[...]
    scale = 1.0 / math.sqrt(head_size)
    lane = lax.broadcasted_iota(jnp.int32, (rows, LANES), 1)

    def attend(sources, blocks, lower, upper, deliver):
        for g in range(group):
            for t, source in enumerate(sources):
                qs[(g * 4 + t) * rows : (g * 4 + t + 1) * rows, :] = source[
                    :, g * head_size : (g + 1) * head_size
                ]
        per = 2
        chunk = per * 4 * rows
        for c in range(group // per):
            block_queries = qs[c * chunk : (c + 1) * chunk, :]
            parts = []
            for b in blocks:
                position = first + b * reach + lax.broadcasted_iota(jnp.int32, (1, reach), 1)
                bias = jnp.where((position >= lower) & (position < upper), 0.0, NEGATIVE)
                scores = dot_nt(block_queries, kcat[b * reach : (b + 1) * reach, :]) + bias
                top = jnp.max(scores, axis=1, keepdims=True)
                weights = jnp.exp2((scores - top) * (scale * LOG2E))
                total = jnp.sum(weights, axis=1, keepdims=True)
                out = jnp.dot(
                    weights.astype(jnp.bfloat16),
                    vcat[b * reach : (b + 1) * reach, :],
                    preferred_element_type=jnp.float32,
                )
                parts.append((out / total, top * scale + jnp.log(total)))
            out, lse = parts[0]
            if len(parts) > 1:
                joint = jnp.maximum(parts[0][1], parts[1][1])
                left = jnp.exp(parts[0][1] - joint)
                right = jnp.exp(parts[1][1] - joint)
                total = left + right
                out = parts[0][0] * (left / total) + parts[1][0] * (right / total)
                lse = joint + jnp.log(total)
            for gg in range(per):
                g = c * per + gg
                for t in range(4):
                    at = (gg * 4 + t) * rows
                    deliver(t, g, out[at : at + rows], lse[at : at + rows])

    def place(ref, g):
        return ref, pl.ds(pl.multiple_of(step * columns + g * head_size, LANES), head_size)

    def encode(ref, side_ref, t, g, out, lse):
        head = step * group + g
        peak = jnp.max(jnp.abs(out), axis=1, keepdims=True)
        power = jnp.ceil(jnp.clip(jnp.log(jnp.maximum(peak, 1e-30)) * LOG2E, -90.0, 20.0))
        coded = jnp.round(out * (jnp.exp2(-power) * WIRE_TOP))
        target, where = place(ref, g)
        target[:, where] = coded.astype(jnp.int32).astype(WIRE)
        eighths = jnp.maximum(lse, -4000.0) * 8.0
        whole = jnp.floor(eighths)
        fraction = jnp.round((eighths - whole) * FRACTION_TOP)
        at = slice(t * rows, (t + 1) * rows)
        held = side_ref[at, :]
        held = jnp.where(lane == head, whole, held)
        held = jnp.where(lane == heads + head, fraction, held)
        side_ref[at, :] = jnp.where(lane == 2 * heads + head, power, held)

    def deliver_main(t, g, out, lse):
        if t == 0:
            target, where = place(own_out, g)
            target[:, where] = out
            own_side[...] = jnp.where(lane == step * group + g, lse, own_side[...])
        else:
            encode(outs[t - 1], side, t - 1, g, out, lse)

    def deliver_extra(t, g, out, lse):
        encode(extra_outs[t], extra_side, t, g, out, lse)

    @pl.when(step == 0)
    def _():
        own_side[...] = jnp.zeros_like(own_side)
        side[...] = jnp.zeros_like(side)
        extra_side[...] = jnp.zeros_like(extra_side)

    attend(queries, (0, 1), low, high, deliver_main)
    straddles = chip == lax.axis_size("kv") // 4 - 1

    @pl.when(straddles)
    def _():
        attend(extras, (1,), starts[1], ends[1], deliver_extra)

    @pl.when(step == pl.num_programs(0) - 1)
    def _():
        width = heads * head_size
        own_out[:, width:] = own_side[...]
        for t, ref in enumerate(outs):
            ref[:, width:] = side[t * rows : (t + 1) * rows, :].astype(jnp.int32).astype(WIRE)
        for t, ref in enumerate(extra_outs):
            ref[:, width:] = extra_side[t * rows : (t + 1) * rows, :].astype(jnp.int32).astype(WIRE)


def merge_kernel(own_ref, near_ref, far_ref, both_ref, x_local, x_a, x_b, x_c, keep_ref, send_ref, x_ref):
    rows, padded = own_ref.shape
    width = padded - LANES
    head_size = HEAD_SIZE
    heads = width // head_size
    half = rows // 2
    chip = lax.axis_index("kv") // 2
    chips = lax.axis_size("kv") // 2
    for at, ref in enumerate((x_a, x_local, x_b, x_c)):

        @pl.when(chip == at)
        def _():
            x_ref[...] = ref[...]

    def decoded(ref):
        side = ref[:, width:].astype(jnp.int32).astype(jnp.float32)
        lse = (side[:, :heads] + side[:, heads : 2 * heads] * (1.0 / FRACTION_TOP)) * 0.125
        return lse, jnp.exp2(side[:, 2 * heads : 3 * heads]) * (1.0 / WIRE_TOP), ref

    own = (own_ref[:, width : width + heads], None, own_ref)
    x = decoded(x_ref)
    upper = chip >= chips // 2
    absent = jnp.full_like(x[0], NEGATIVE)
    for at, parts in (
        (0, (own, decoded(near_ref), (jnp.where(upper, x[0], absent), x[1], x[2]))),
        (half, (decoded(far_ref), decoded(both_ref), (jnp.where(upper, absent, x[0]), x[1], x[2]))),
    ):
        joint = functools.reduce(jnp.maximum, [part[0] for part in parts])
        factors = [jnp.exp(part[0] - joint) for part in parts]
        total = functools.reduce(jnp.add, factors)
        shares = [
            factor / total if part[1] is None else factor / total * part[1]
            for factor, part in zip(factors, parts)
        ]
        lse = joint + jnp.log(total)
        lse = jnp.concatenate([lse, jnp.zeros((rows, LANES - heads), jnp.float32)], axis=1)
        keep_ref[at : at + half, width:] = lse[:half]
        send_ref[at : at + half, width:] = lse[half:]
        for h in range(heads):
            columns = slice(h * head_size, (h + 1) * head_size)
            out = jnp.zeros((rows, head_size), jnp.float32)
            for share, part in zip(shares, parts):
                held = part[2][:, columns]
                if part[1] is not None:
                    held = held.astype(jnp.int32).astype(jnp.float32)
                out = out + share[:, h : h + 1] * held
            keep_ref[at : at + half, columns] = out[:half]
            send_ref[at : at + half, columns] = out[half:]


def final_kernel(prompt_ref, keep_ref, recv_ref, so_a, sl_a, so_b, sl_b, out_ref, acc):
    seqs, width = out_ref.shape
    half_width = keep_ref.shape[1] - LANES
    heads = half_width // HEAD_SIZE
    half = seqs // 2
    core = lax.axis_index("kv") % 2
    for ref, which in ((keep_ref, core), (recv_ref, 1 - core)):
        for h in range(heads):
            where = pl.ds(pl.multiple_of(which * half_width + h * HEAD_SIZE, LANES), HEAD_SIZE)
            for at, so, sl in ((0, so_a, sl_a), (half, so_b, sl_b)):
                lse = ref[at : at + half, half_width + h : half_width + h + 1]
                suffix_lse = sl[:, where]
                joint = jnp.maximum(lse, suffix_lse)
                left = jnp.exp(lse - joint)
                right = jnp.exp(suffix_lse - joint)
                held = ref[at : at + half, h * HEAD_SIZE : (h + 1) * HEAD_SIZE]
                acc[at : at + half, where] = (left * held + right * so[:, where]) / (left + right)

    dests = []
    packed_places(prompt_ref, seqs, own_group(), lambda i, d: dests.append(d))
    for i, d in enumerate(dests):
        out_ref[i : i + 1, :] = acc[pl.ds(d, 1), :]


def split_heads_shards(
    queries,
    prompt_of,
    prompt_len,
    suffix_len,
    page_table,
    prompt_keys,
    shared_prompt_values,
    suffix_pool_keys,
    suffix_pool_values,
):
    kv_count = lax.axis_size("kv")
    seqs, width = queries.shape
    heads = width // HEAD_SIZE
    half_width = width // 2
    reach, local_width = prompt_keys.shape
    kv_heads = local_width // HEAD_SIZE
    slots = page_table.shape[1]
    page = suffix_pool_keys.shape[1]
    half = seqs // 2
    padded = half_width + LANES
    prompts = prompt_of.reshape(-1)
    smem = pl.BlockSpec(memory_space=pltpu.SMEM)
    vmem = pl.BlockSpec(memory_space=pltpu.VMEM)
    hbm = pl.BlockSpec(memory_space=pl.ANY)
    core_swap = [(i, i ^ 1) for i in range(kv_count)]

    def hop(value, mask):
        return lax.ppermute(value, "kv", [(i, i ^ mask) for i in range(kv_count)])

    def chip_hop(value, source, target):
        return lax.ppermute(value, "kv", [(2 * source + c, 2 * target + c) for c in range(2)])

    def struct(shape, dtype):
        return jax.ShapeDtypeStruct(shape, dtype)

    keys_other = lax.ppermute(prompt_keys, "kv", core_swap)
    values_other = lax.ppermute(shared_prompt_values, "kv", core_swap)
    rows_half = struct((seqs, half_width), jnp.bfloat16)
    keep, send = pl.pallas_call(
        pack_kernel, out_shape=(rows_half, rows_half), in_specs=[smem, vmem], name="pack"
    )(prompts, queries)
    received = hop(send, 1)
    main, cross = pl.pallas_call(build_kernel, out_shape=(rows_half, rows_half), name="build")(
        keep, received
    )
    main_far = hop(cross, 4)
    main_near = hop(main, 2)
    edge = kv_count // 4 - 1
    others = [chip for chip in range(kv_count // 2) if chip != edge]
    extra_queries = [cross] + [
        chip_hop(cross if chip <= edge else main, chip, edge) for chip in others
    ]
    suffix_queries = queries.reshape(seqs, heads, HEAD_SIZE)

    def suffix(first):
        return pl.pallas_call(
            functools.partial(suffix_kernel, first),
            out_shape=(struct((half, width), jnp.float32), struct((half, width), jnp.float32)),
            in_specs=[smem, smem, smem, vmem, hbm, hbm],
            scratch_shapes=[
                pltpu.SMEM((seqs,), jnp.int32),
                pltpu.VMEM((half, slots, page, local_width), jnp.bfloat16),
                pltpu.VMEM((half, slots, page, local_width), jnp.bfloat16),
                pltpu.SemaphoreType.DMA((half,)),
                pltpu.SemaphoreType.DMA((half,)),
            ],
            cost_estimate=pl.CostEstimate(
                flops=4 * 1000 * half * heads * slots * page * HEAD_SIZE,
                transcendentals=half * heads * slots * page,
                bytes_accessed=4 * half * slots * page * local_width,
            ),
            name=f"suffix{first}",
        )(prompts, page_table, suffix_len, suffix_queries, suffix_pool_keys, suffix_pool_values)

    suffix_a = suffix(0)
    main_both = hop(main_far, 2)
    suffix_b = suffix(half)

    steps = kv_heads // 2
    columns = half_width // steps
    row_block = pl.BlockSpec((seqs, columns), lambda j, core: (0, j))
    cache_block = pl.BlockSpec((reach, HEAD_SIZE), lambda j, core: (0, core[0] * steps + j))
    whole = pl.BlockSpec((seqs, padded), lambda j, core: (0, 0))
    core = (lax.axis_index("kv") % 2).astype(jnp.int32).reshape(1)
    coded = struct((seqs, padded), WIRE)
    results = pl.pallas_call(
        prompt_kernel,
        grid_spec=pltpu.PrefetchScalarGridSpec(
            num_scalar_prefetch=1,
            grid=(steps,),
            in_specs=[pl.BlockSpec(memory_space=pltpu.SMEM)] + [row_block] * 8 + [cache_block] * 4,
            out_specs=[whole] * 8,
            scratch_shapes=[
                pltpu.VMEM((2 * reach, HEAD_SIZE), jnp.bfloat16),
                pltpu.VMEM((2 * reach, HEAD_SIZE), jnp.bfloat16),
                pltpu.VMEM((4 * seqs * columns // HEAD_SIZE, HEAD_SIZE), jnp.bfloat16),
                pltpu.VMEM((seqs, LANES), jnp.float32),
                pltpu.VMEM((3 * seqs, LANES), jnp.float32),
                pltpu.VMEM((4 * seqs, LANES), jnp.float32),
            ],
        ),
        out_shape=[struct((seqs, padded), jnp.float32)] + [coded] * 7,
        name="prompt",
    )(
        core,
        prompt_len,
        main,
        main_near,
        main_far,
        main_both,
        *extra_queries,
        prompt_keys,
        keys_other,
        shared_prompt_values,
        values_other,
    )
    own, to_near, to_far, to_both = results[:4]
    extra_local, extra_out = results[4], results[5:]
    near, far, both = hop(to_near, 2), hop(to_far, 4), hop(to_both, 6)
    extra_in = [chip_hop(value, edge, chip) for value, chip in zip(extra_out, others)]
    joined_rows = struct((seqs, padded), jnp.float32)
    kept, sent = pl.pallas_call(
        merge_kernel,
        out_shape=(joined_rows, joined_rows),
        scratch_shapes=[pltpu.VMEM((seqs, padded), WIRE)],
        name="merge",
    )(own, near, far, both, extra_local, *extra_in)
    returned = hop(sent, 1)
    return pl.pallas_call(
        final_kernel,
        out_shape=struct((seqs, width), jnp.float32),
        in_specs=[smem] + [vmem] * 6,
        scratch_shapes=[pltpu.VMEM((seqs, width), jnp.float32)],
        name="final",
    )(prompts, kept, returned, *suffix_a, *suffix_b)


def splits_heads(mesh, prompt_len):
    prompts = prompt_len.shape[0] // mesh.shape["grp"]
    return mesh.shape["sub"] == 1 and mesh.shape["kv"] == 4 * prompts and prompts == 2


def solution(mesh):
    placed = (
        P(("grp", "kv"), "hd"),
        P("grp", None),
        P("grp"),
        P(("grp", "kv")),
        P(("grp", "kv"), "sub"),
        P(("grp", "kv", "sub"), "hd"),
        P(("grp", "kv", "sub"), "hd"),
        P(("grp", "kv", "sub"), None, "hd"),
        P(("grp", "kv", "sub"), None, "hd"),
    )

    def run(*arrays):
        body = split_heads_shards if splits_heads(mesh, arrays[2]) else shards
        return jax.shard_map(
            body, mesh=mesh, in_specs=placed, out_specs=P(("grp", "kv"), "hd"), check_vma=False
        )(*arrays)

    return run
```
